8 devices in a mesh: dp: 1 (over z), tp: 8 (over y, x, core).
Axes of the slice: x: 2, y: 2, z: 1, core: 2. Of those that a mesh axis runs over, the one named last changes fastest.
Arguments:
- hidden: bfloat16 [512, 1024], P('dp')
- positions: int32 [512], P('dp')
- ln1_gain: float32 [2, 1024], replicated
- ln1_bias: float32 [2, 1024], replicated
- ln2_gain: float32 [2, 1024], replicated
- ln2_bias: float32 [2, 1024], replicated
- w_qkv: bfloat16 [2, 1024, 3072], P(None, None, 'tp')
- b_qkv: bfloat16 [2, 3072], P(None, 'tp')
- w_out: bfloat16 [2, 1024, 1024], P(None, 'tp')
- b_out: bfloat16 [2, 1024], replicated
- w_up: bfloat16 [2, 1024, 4096], P(None, None, 'tp')
- b_up: bfloat16 [2, 4096], P(None, 'tp')
- w_down: bfloat16 [2, 4096, 1024], P(None, 'tp')
- b_down: bfloat16 [2, 1024], replicated
- k_cache: bfloat16 [2, 512, 16, 128, 64], P(None, 'dp', 'tp')
- v_cache: bfloat16 [2, 512, 16, 128, 64], P(None, 'dp', 'tp')
Outputs:
- output 1: bfloat16 [512, 1024], P('dp')
- output 2: bfloat16 [2, 512, 16, 128, 64], P(None, 'dp', 'tp')
- output 3: bfloat16 [2, 512, 16, 128, 64], P(None, 'dp', 'tp')
All inputs are finite; a program needn't handle non-finite values.
Results may differ from the reference program's by a relative error of at most 0.0118106.
Values are sent between devices in bfloat16 or wider.
A program may use at most 1 GiB of HBM per device.

```python
import jax
import jax.numpy as jnp
from jax import lax

D = 1024
HEADS = 16
HEAD = 64
FF = 4096
LAYERS = 2
B = 512
S = 128

ROT = HEAD // 4
HALF = HEAD // 8
QKV = 3 * HEADS * HEAD
INNER = HEADS * HEAD
EPS = 1e-5


def setup_inputs(seed: int = 0, part: int = 0) -> dict:
    base_key = jax.random.key(seed)
    w_keys = jax.random.split(base_key, 12)
    p_keys = jax.random.split(jax.random.fold_in(base_key, part), 6)
    normal = jax.random.normal
    row_mean = normal(p_keys[0], (B, 1), jnp.float32)
    row_scale = jax.random.uniform(p_keys[1], (B, 1), jnp.float32, 0.5, 2.0)
    hidden = ((normal(p_keys[2], (B, D), jnp.float32) + row_mean) * row_scale).astype(jnp.bfloat16)
    pos_draw = jax.random.randint(p_keys[3], (B,), 0, S)
    positions = jnp.where(jnp.arange(B) == 0, S - 1, pos_draw).astype(jnp.int32)
    cache_shape = (LAYERS, B, HEADS, S, HEAD)
    k_cache = (2.5 * normal(p_keys[4], cache_shape, jnp.float32)).astype(jnp.bfloat16)
    v_cache = normal(p_keys[5], cache_shape, jnp.float32).astype(jnp.bfloat16)
    return dict(
        hidden=hidden,
        positions=positions,
        ln1_gain=1.0 + 0.3 * normal(w_keys[0], (LAYERS, D), jnp.float32),
        ln1_bias=0.3 * normal(w_keys[1], (LAYERS, D), jnp.float32),
        ln2_gain=1.0 + 0.3 * normal(w_keys[2], (LAYERS, D), jnp.float32),
        ln2_bias=0.3 * normal(w_keys[3], (LAYERS, D), jnp.float32),
        w_qkv=(normal(w_keys[4], (LAYERS, D, QKV), jnp.float32) * D ** -0.5).astype(jnp.bfloat16),
        b_qkv=(0.5 * normal(w_keys[5], (LAYERS, QKV), jnp.float32)).astype(jnp.bfloat16),
        w_out=(normal(w_keys[6], (LAYERS, INNER, D), jnp.float32) * INNER ** -0.5).astype(jnp.bfloat16),
        b_out=(0.5 * normal(w_keys[7], (LAYERS, D), jnp.float32)).astype(jnp.bfloat16),
        w_up=(normal(w_keys[8], (LAYERS, D, FF), jnp.float32) * D ** -0.5).astype(jnp.bfloat16),
        b_up=(0.5 * normal(w_keys[9], (LAYERS, FF), jnp.float32)).astype(jnp.bfloat16),
        w_down=(normal(w_keys[10], (LAYERS, FF, D), jnp.float32) * FF ** -0.5).astype(jnp.bfloat16),
        b_down=(0.5 * normal(w_keys[11], (LAYERS, D), jnp.float32)).astype(jnp.bfloat16),
        k_cache=k_cache,
        v_cache=v_cache,
    )


def layer_norm(hid_f32, gain, bias):
    mean_val = jnp.mean(hid_f32, axis=-1, keepdims=True)
    centered = hid_f32 - mean_val
    variance = jnp.mean(centered * centered, axis=-1, keepdims=True)
    return (centered * lax.rsqrt(variance + EPS) * gain + bias).astype(jnp.bfloat16)


def rotary(vecs, positions):
    inv_freq = 10000.0 ** (-2.0 * jnp.arange(HALF, dtype=jnp.float32) / ROT)
    angle = positions.astype(jnp.float32)[:, None, None] * inv_freq
    cos_a = jnp.cos(angle)
    sin_a = jnp.sin(angle)
    first = vecs[..., :HALF]
    second = vecs[..., HALF:ROT]
    return jnp.concatenate([first * cos_a - second * sin_a, second * cos_a + first * sin_a, vecs[..., ROT:]], axis=-1)


def attend_row(row_data):
    query, k_row, v_row, position = row_data
    scores = jnp.einsum('hd,hsd->hs', query.astype(jnp.float32), k_row.astype(jnp.float32)) * HEAD ** -0.5
    scores = jnp.where(jnp.arange(S)[None, :] <= position, scores, -1e30)
    attn_prob = jax.nn.softmax(scores, axis=-1).astype(jnp.bfloat16)
    context = jnp.einsum('hs,hsd->hd', attn_prob.astype(jnp.float32), v_row.astype(jnp.float32))
    return context.astype(jnp.bfloat16)


def decode_layer(hidden, positions, layer):
    ln1_gain, ln1_bias, ln2_gain, ln2_bias, w_qkv, b_qkv, w_out, b_out, w_up, b_up, w_down, b_down, k_layer, v_layer = layer
    hid_f32 = hidden.astype(jnp.float32)
    attn_in = layer_norm(hid_f32, ln1_gain, ln1_bias)
    mlp_in = layer_norm(hid_f32, ln2_gain, ln2_bias)
    qkv_proj = (jnp.dot(attn_in, w_qkv, preferred_element_type=jnp.float32) + b_qkv.astype(jnp.float32)).astype(jnp.bfloat16)
    qkv_proj = qkv_proj.reshape(B, HEADS, 3, HEAD).astype(jnp.float32)
    query = rotary(qkv_proj[:, :, 0], positions).astype(jnp.bfloat16)
    key_new = rotary(qkv_proj[:, :, 1], positions).astype(jnp.bfloat16)
    value_new = qkv_proj[:, :, 2].astype(jnp.bfloat16)
    slot_hit = (jnp.arange(S)[None, :] == positions[:, None])[:, None, :, None]
    k_layer = jnp.where(slot_hit, key_new[:, :, None, :], k_layer)
    v_layer = jnp.where(slot_hit, value_new[:, :, None, :], v_layer)
    context = lax.map(attend_row, (query, k_layer, v_layer, positions))
    attn_sum = jnp.dot(context.reshape(B, INNER), w_out, preferred_element_type=jnp.float32)
    up_proj = jnp.dot(mlp_in, w_up, preferred_element_type=jnp.float32) + b_up.astype(jnp.float32)
    gelu_out = jax.nn.gelu(up_proj, approximate=False).astype(jnp.bfloat16)
    mlp_sum = jnp.dot(gelu_out, w_down, preferred_element_type=jnp.float32)
    total = hid_f32 + attn_sum + mlp_sum + b_out.astype(jnp.float32) + b_down.astype(jnp.float32)
    return total.astype(jnp.bfloat16), k_layer, v_layer


def reference(hidden, positions, ln1_gain, ln1_bias, ln2_gain, ln2_bias, w_qkv, b_qkv, w_out, b_out, w_up, b_up, w_down, b_down, k_cache, v_cache):
    def body(carry, layer):
        new_hidden, k_layer, v_layer = decode_layer(carry, positions, layer)
        return new_hidden, (k_layer, v_layer)
    stacks = (ln1_gain, ln1_bias, ln2_gain, ln2_bias, w_qkv, b_qkv, w_out, b_out, w_up, b_up, w_down, b_down, k_cache, v_cache)
    hidden_out, caches = lax.scan(body, hidden, stacks)
    return hidden_out, caches[0], caches[1]
```

```python
import functools

import jax
import jax.numpy as jnp
import numpy as np
from jax import lax
from jax.experimental import pallas as pl
from jax.experimental.pallas import tpu as pltpu
from jax.sharding import PartitionSpec as P

EPS = 1e-5
BF = jnp.bfloat16
F32 = jnp.float32
MESH = pl.DeviceIdType.MESH
LANES = 128
BLOCK = 32
SLOTS = 8
AHEAD = 5
CHUNK = 128


def iota(shape, dim):
    return lax.broadcasted_iota(jnp.int32, shape, dim)


def normalize(hid):
    mean_val = jnp.mean(hid, axis=-1, keepdims=True)
    centered = hid - mean_val
    variance = jnp.mean(centered * centered, axis=-1, keepdims=True)
    return centered * lax.rsqrt(variance + EPS)


def rotary_tables(pos_row, head):
    pos = jnp.transpose(jnp.broadcast_to(pos_row.astype(F32), (CHUNK, LANES)))
    dim = iota((CHUNK, LANES), 1) % head
    half = head // 8
    freq = np.float64(10000.0) ** (-2.0 * np.arange(half) / (2 * half))
    which = dim % half
    inv = jnp.full((CHUNK, LANES), np.float32(freq[0]), F32)
    for i in range(1, half):
        inv = jnp.where(which == i, np.float32(freq[i]), inv)
    angle = pos * inv
    cos_a = jnp.cos(angle)
    sin_a = jnp.sin(angle)
    cos_t = jnp.where(dim < 2 * half, cos_a, 1.0)
    sin_lo = jnp.where(dim < half, -sin_a, 0.0)
    sin_hi = jnp.where((dim >= half) & (dim < 2 * half), sin_a, 0.0)
    return pos, cos_t, sin_lo, sin_hi


def rotate(x, tables, half):
    cos_t, sin_lo, sin_hi = tables
    up = pltpu.roll(x, LANES - half, 1)
    down = pltpu.roll(x, half, 1)
    return x * cos_t + up * sin_lo + down * sin_hi


def attend_kernel(layer, num_rows, head, *refs):
    (pos_ref, hid_any, gain_ref, bias_ref, w_any, b_ref, k_in, v_in) = refs[:8]
    refs = refs[8:]
    if layer > 0:
        refs = refs[2:]
    (k_out, v_out, ctx_ref, hid_s, w_s, q_s, pos_s, kn_s, vn_s, k_buf, v_buf, rd_sem, wr_sem, in_sem) = refs
    num_blocks = num_rows // BLOCK
    per_chunk = CHUNK // BLOCK

    def reads(blk, slot):
        rows = pl.ds(blk * BLOCK, BLOCK)
        return (pltpu.make_async_copy(k_in.at[layer, rows], k_buf.at[slot], rd_sem.at[0, slot]),
                pltpu.make_async_copy(v_in.at[layer, rows], v_buf.at[slot], rd_sem.at[1, slot]))

    def writes(blk, slot):
        rows = pl.ds(blk * BLOCK, BLOCK)
        return (pltpu.make_async_copy(k_buf.at[slot], k_out.at[layer, rows], wr_sem.at[0, slot]),
                pltpu.make_async_copy(v_buf.at[slot], v_out.at[layer, rows], wr_sem.at[1, slot]))

    hid_copy = pltpu.make_async_copy(hid_any, hid_s, in_sem.at[0])
    w_copy = pltpu.make_async_copy(w_any.at[layer], w_s, in_sem.at[1])
    hid_copy.start()
    w_copy.start()
    for blk in range(SLOTS):
        for copy in reads(blk, blk):
            copy.start()
    hid_copy.wait()
    w_copy.wait()

    lane = iota((CHUNK, LANES), 1)
    low = lane < head

    @pl.loop(0, num_rows // CHUNK)
    def _(c):
        rows = pl.ds(pl.multiple_of(c * CHUNK, CHUNK), CHUNK)
        pos, *tables = rotary_tables(pos_ref[pl.ds(c, 1), :], head)
        pos_s[rows, :] = pos
        normed = normalize(hid_s[rows, :].astype(F32))
        attn_in = (normed * gain_ref[layer:layer + 1, :] + bias_ref[layer:layer + 1, :]).astype(BF)
        qkv = jnp.dot(attn_in, w_s[...], preferred_element_type=F32) + b_ref[layer:layer + 1, :].astype(F32)
        qkv = qkv.astype(BF).astype(F32)
        one, two, three = qkv[:, :LANES], qkv[:, LANES:2 * LANES], qkv[:, 2 * LANES:]
        query = jnp.where(low, one, two)
        key = pltpu.roll(jnp.where(low, three, one), head, 1)
        value = jnp.where(low, two, three)
        q_s[rows, :] = rotate(query, tables, head // 8).astype(BF).astype(F32)
        key_t = jnp.transpose(rotate(key, tables, head // 8).astype(BF).astype(F32))
        val_t = jnp.transpose(value)
        for i in range(per_chunk):
            kn_s[c * per_chunk + i] = (pltpu.roll(key_t, (LANES - i * BLOCK) % LANES, 1) if i else key_t).astype(kn_s.dtype)
            vn_s[c * per_chunk + i] = (pltpu.roll(val_t, (LANES - i * BLOCK) % LANES, 1) if i else val_t).astype(vn_s.dtype)

    scale = head ** -0.5
    sub16 = iota((16, LANES), 0) % 8
    lane16 = iota((16, LANES), 1)
    lane8 = iota((8, LANES), 1)
    even = (sub16 % 2) == 0
    first = sub16 < 4
    upper = (sub16 % 4) < 2

    def merged(buf, new_s, slot, blk, j, hit):
        col = jnp.broadcast_to(new_s[blk][:, j:j + 1], (LANES, LANES)).astype(BF)
        out = jnp.where(hit, col, buf[slot, j])
        buf[slot, j] = out
        return out

    def square(tiles):
        return jnp.concatenate([jnp.concatenate(tiles[:2], 1), jnp.concatenate(tiles[2:], 1)], 0)

    @pl.loop(0, num_blocks)
    def _(blk):
        slot = lax.rem(blk, SLOTS)

        @pl.when((blk + AHEAD >= SLOTS) & (blk + AHEAD < num_blocks))
        def _():
            ahead = blk + AHEAD
            ahead_slot = lax.rem(ahead, SLOTS)
            for copy in writes(ahead - SLOTS, ahead_slot):
                copy.wait()
            for copy in reads(ahead, ahead_slot):
                copy.start()

        for copy in reads(blk, slot):
            copy.wait()

        base = pl.multiple_of(blk * BLOCK, BLOCK)
        for g in range(BLOCK // 8):
            rows = pl.ds(base + 8 * g, 8)
            q8 = q_s[rows, :]
            p8 = pos_s[rows, :]
            hits = [lane.astype(BF) == jnp.broadcast_to(p8[j:j + 1, :], (LANES, LANES)).astype(BF) for j in range(8)]
            q16 = jnp.concatenate([jnp.where(lane8 < head, q8, 0.0), jnp.where(lane8 < head, 0.0, q8)], 0)
            p16 = jnp.concatenate([p8, p8], 0)
            scores = []
            for t in range(2):
                keys = square([merged(k_buf, kn_s, slot, blk, 8 * g + 4 * t + i, hits[4 * t + i]) for i in range(4)])
                mine = first if t == 0 else ~first
                lhs = jnp.concatenate([jnp.where(mine & upper, q16, 0.0), jnp.where(mine & ~upper, q16, 0.0)], 1).astype(BF)
                out = jnp.dot(lhs, keys, preferred_element_type=F32)
                scores.append(jnp.where(even, out[:, :LANES], out[:, LANES:]))
            s = jnp.where(first, scores[0], scores[1]) * scale
            s = jnp.where(lane16.astype(F32) <= p16, s, -1e30)
            e = jnp.exp(s - jnp.max(s, axis=-1, keepdims=True))
            prob = e / jnp.sum(e, axis=-1, keepdims=True)
            lhs = jnp.concatenate([jnp.where(even, prob, 0.0), jnp.where(even, 0.0, prob)], 1).astype(BF)
            ctx = []
            for t in range(2):
                vals = square([merged(v_buf, vn_s, slot, blk, 8 * g + 4 * t + i, hits[4 * t + i]) for i in range(4)])
                out = lax.dot_general(lhs, vals, (((1,), (1,)), ((), ())), preferred_element_type=F32)
                ctx.append(jnp.where(upper, out[:, :LANES], out[:, LANES:]))
            c16 = jnp.where(first, ctx[0], ctx[1])
            ctx_ref[rows, :] = jnp.where(lane8 < head, c16[:8], c16[8:])

        for copy in writes(blk, slot):
            copy.start()

    for blk in range(num_blocks - SLOTS, num_blocks):
        for copy in writes(blk, blk % SLOTS):
            copy.wait()


def attend(layer, positions, hidden, gain, bias, w_qkv, b_qkv, k_cache, v_cache, prev):
    num_rows, width = hidden.shape
    _, _, inner, slots = k_cache.shape
    head = inner // 2
    num_blocks = num_rows // BLOCK
    vmem = pl.BlockSpec(memory_space=pltpu.VMEM)
    anyspace = pl.BlockSpec(memory_space=pl.ANY)
    operands = [positions, hidden, gain, bias, w_qkv, b_qkv, k_cache, v_cache]
    specs = [vmem, anyspace, vmem, vmem, anyspace, vmem, anyspace, anyspace]
    aliases = {}
    if prev is not None:
        operands += list(prev)
        specs += [anyspace, anyspace]
        aliases = {8: 0, 9: 1}
    cache = jax.ShapeDtypeStruct(k_cache.shape, BF)
    return pl.pallas_call(
        functools.partial(attend_kernel, layer, num_rows, head),
        out_shape=(cache, cache, jax.ShapeDtypeStruct((num_rows, inner), F32)),
        in_specs=specs,
        out_specs=(anyspace, anyspace, vmem),
        scratch_shapes=[
            pltpu.VMEM((num_rows, width), BF),
            pltpu.VMEM(w_qkv.shape[1:], BF),
            pltpu.VMEM((num_rows, LANES), F32),
            pltpu.VMEM((num_rows, LANES), F32),
            pltpu.VMEM((num_blocks, LANES, LANES), F32),
            pltpu.VMEM((num_blocks, LANES, LANES), F32),
            pltpu.VMEM((SLOTS, BLOCK, inner, slots), BF),
            pltpu.VMEM((SLOTS, BLOCK, inner, slots), BF),
            pltpu.SemaphoreType.DMA((2, SLOTS)),
            pltpu.SemaphoreType.DMA((2, SLOTS)),
            pltpu.SemaphoreType.DMA((2,)),
        ],
        input_output_aliases=aliases,
        compiler_params=pltpu.CompilerParams(vmem_limit_bytes=56 * 1024 * 1024),
        name=f"attend{layer}",
    )(*operands)


def combine_kernel(layer, num_rows, hid_ref, ctx_ref, gain_ref, bias_ref, w_out_any, w_up_any, b_up_ref, w_down_any, b_out_ref, b_down_ref,
                   out_ref, w_out, w_up, w_down, part, half, pair_in, quad_in, final, in_sem,
                   pair_send, pair_recv, quad_send, quad_recv, gather_send, gather_recv, fwd_send, fwd_recv):
    me = lax.axis_index("tp")
    core = lax.rem(me, 2)
    chip = lax.div(me, 2)
    partner = me + 1 - 2 * core
    others = []
    for k in range(1, 4):
        x = lax.rem(chip, 2)
        y = lax.div(chip, 2)
        ox = 1 - x if k & 1 else x
        oy = 1 - y if k & 2 else y
        others.append(2 * oy + ox)
    num_chunks = num_rows // CHUNK
    half_rows = CHUNK // 2
    piece = CHUNK // 8

    weights = [pltpu.make_async_copy(src.at[layer], dst, in_sem.at[i])
               for i, (src, dst) in enumerate([(w_up_any, w_up), (w_down_any, w_down), (w_out_any, w_out)])]
    for copy in weights:
        copy.start()

    barrier = pltpu.get_barrier_semaphore()
    peers = [partner] + [2 * o + core for o in others]
    for peer in peers:
        pl.semaphore_signal(barrier, inc=1, device_id={"tp": peer}, device_id_type=MESH)

    def remote(src, dst, send, recv, device):
        return pltpu.make_async_remote_copy(src_ref=src, dst_ref=dst, send_sem=send, recv_sem=recv,
                                            device_id={"tp": device}, device_id_type=MESH)

    def pair_copy(c):
        start = pl.multiple_of((1 - core) * half_rows, half_rows)
        return remote(part.at[c, pl.ds(start, half_rows)], pair_in.at[c], pair_send.at[c], pair_recv.at[c], partner)

    def quad_copy(c, k):
        start = pl.multiple_of(others[k] * piece, piece)
        return remote(half.at[c, pl.ds(start, piece)], quad_in.at[c, k], quad_send.at[c, k], quad_recv.at[c, k], 2 * others[k] + core)

    def piece_rows(c, owner_core, owner_chip):
        return pl.ds(pl.multiple_of(c * CHUNK + owner_core * half_rows + owner_chip * piece, piece), piece)

    def gather_copy(c, k):
        rows = piece_rows(c, core, chip)
        return remote(final.at[rows], final.at[rows], gather_send.at[c, k], gather_recv.at[c, k], 2 * others[k] + core)

    def fwd_copy(c):
        rows = pl.ds(pl.multiple_of(c * CHUNK + core * half_rows, half_rows), half_rows)
        return remote(final.at[rows], final.at[rows], fwd_send.at[c], fwd_recv.at[c], partner)

    def compute(c):
        rows = pl.ds(c * CHUNK, CHUNK)
        normed = normalize(hid_ref[rows, :].astype(F32))
        mlp_in = (normed * gain_ref[layer:layer + 1, :] + bias_ref[layer:layer + 1, :]).astype(BF)
        up = jnp.dot(mlp_in, w_up[...], preferred_element_type=F32) + b_up_ref[layer:layer + 1, :].astype(F32)
        act = (0.5 * up * (1.0 + lax.erf(up * np.float32(np.sqrt(0.5))))).astype(BF)
        total = jnp.dot(act, w_down[...], preferred_element_type=F32)
        total = total + jnp.dot(ctx_ref[rows, :].astype(BF), w_out[...], preferred_element_type=F32)
        part[c] = total.astype(BF)

    def pair_done(c):
        pair_copy(c).wait()
        mine = pl.ds(pl.multiple_of(core * half_rows, half_rows), half_rows)
        half[c] = (part[c, mine, :].astype(F32) + pair_in[c].astype(F32)).astype(BF)

    def quad_done(c):
        for k in range(3):
            quad_copy(c, k).wait()
        mine = pl.ds(pl.multiple_of(chip * piece, piece), piece)
        rows = piece_rows(c, core, chip)
        total = hid_ref[rows, :].astype(F32) + half[c, mine, :].astype(F32)
        for k in range(3):
            total = total + quad_in[c, k].astype(F32)
        total = total + b_out_ref[layer:layer + 1, :].astype(F32) + b_down_ref[layer:layer + 1, :].astype(F32)
        final[rows, :] = total.astype(BF)

    for copy in weights:
        copy.wait()
    for step in range(num_chunks + 4):
        if step < num_chunks:
            compute(step)
            if step == 0:
                pl.semaphore_wait(barrier, len(peers))
            pair_copy(step).start()
        if 0 <= step - 1 < num_chunks:
            pair_done(step - 1)
            for k in range(3):
                quad_copy(step - 1, k).start()
        if 0 <= step - 2 < num_chunks:
            quad_done(step - 2)
            for k in range(3):
                gather_copy(step - 2, k).start()
        if 0 <= step - 3 < num_chunks:
            for k in range(3):
                gather_copy(step - 3, k).wait()
            fwd_copy(step - 3).start()
        if 0 <= step - 4 < num_chunks:
            fwd_copy(step - 4).wait()
            rows = pl.ds((step - 4) * CHUNK, CHUNK)
            out_ref[rows, :] = final[rows, :]


def combine(layer, hidden, ctx, gain, bias, w_out, w_up, b_up, w_down, b_out, b_down):
    num_rows, width = hidden.shape
    num_chunks = num_rows // CHUNK
    vmem = pl.BlockSpec(memory_space=pltpu.VMEM)
    anyspace = pl.BlockSpec(memory_space=pl.ANY)
    dma = pltpu.SemaphoreType.DMA
    return pl.pallas_call(
        functools.partial(combine_kernel, layer, num_rows),
        out_shape=jax.ShapeDtypeStruct((num_rows, width), BF),
        in_specs=[vmem, vmem, vmem, vmem, anyspace, anyspace, vmem, anyspace, vmem, vmem],
        out_specs=vmem,
        scratch_shapes=[
            pltpu.VMEM(w_out.shape[1:], BF),
            pltpu.VMEM(w_up.shape[1:], BF),
            pltpu.VMEM(w_down.shape[1:], BF),
            pltpu.VMEM((num_chunks, CHUNK, width), BF),
            pltpu.VMEM((num_chunks, CHUNK // 2, width), BF),
            pltpu.VMEM((num_chunks, CHUNK // 2, width), BF),
            pltpu.VMEM((num_chunks, 3, CHUNK // 8, width), BF),
            pltpu.VMEM((num_rows, width), BF),
            dma((3,)),
            dma((num_chunks,)), dma((num_chunks,)),
            dma((num_chunks, 3)), dma((num_chunks, 3)),
            dma((num_chunks, 3)), dma((num_chunks, 3)),
            dma((num_chunks,)), dma((num_chunks,)),
        ],
        compiler_params=pltpu.CompilerParams(collective_id=layer, has_side_effects=True, vmem_limit_bytes=48 * 1024 * 1024),
        name=f"combine{layer}",
    )(hidden, ctx, gain, bias, w_out, w_up, b_up, w_down, b_out, b_down)


def solution(mesh):
    cache_spec = P(None, 'dp', 'tp', None, None)
    rep_spec = P(None, None)
    in_specs = (P('dp', None), P('dp'), rep_spec, rep_spec, rep_spec, rep_spec,
                P(None, None, 'tp'), P(None, 'tp'), P(None, 'tp', None), rep_spec,
                P(None, None, 'tp'), P(None, 'tp'), P(None, 'tp', None), rep_spec,
                cache_spec, cache_spec)
    out_specs = (P('dp', None), cache_spec, cache_spec)

    def local(hidden, positions, ln1_gain, ln1_bias, ln2_gain, ln2_bias, w_qkv, b_qkv, w_out, b_out, w_up, b_up, w_down, b_down, k_cache, v_cache):
        num_layers, num_rows, heads_local, slots, head_dim = k_cache.shape
        flat = (num_layers, num_rows, heads_local * head_dim, slots)
        k_flat = jnp.swapaxes(k_cache, 3, 4).reshape(flat)
        v_flat = jnp.swapaxes(v_cache, 3, 4).reshape(flat)
        pos = positions.reshape(num_rows // CHUNK, CHUNK)
        prev = None
        for layer in range(num_layers):
            k_out, v_out, ctx = attend(layer, pos, hidden, ln1_gain, ln1_bias, w_qkv, b_qkv, k_flat, v_flat, prev)
            prev = (k_out, v_out)
            hidden = combine(layer, hidden, ctx, ln2_gain, ln2_bias, w_out, w_up, b_up, w_down, b_out, b_down)
        shape = (num_layers, num_rows, heads_local, head_dim, slots)
        return hidden, jnp.swapaxes(prev[0].reshape(shape), 3, 4), jnp.swapaxes(prev[1].reshape(shape), 3, 4)

    return jax.shard_map(local, mesh=mesh, in_specs=in_specs, out_specs=out_specs, check_vma=False)
```

```python
import functools

import jax
import jax.numpy as jnp
import numpy as np
from jax import lax
from jax.experimental import pallas as pl
from jax.experimental.pallas import tpu as pltpu
from jax.sharding import PartitionSpec as P

EPS = 1e-5
BF = jnp.bfloat16
F32 = jnp.float32
MESH = pl.DeviceIdType.MESH
LANES = 128
BLOCK = 32
SLOTS = 8
AHEAD = 5
CHUNK = 128


def iota(shape, dim):
    return lax.broadcasted_iota(jnp.int32, shape, dim)


def normalize(hid):
    mean_val = jnp.mean(hid, axis=-1, keepdims=True)
    centered = hid - mean_val
    variance = jnp.mean(centered * centered, axis=-1, keepdims=True)
    return centered * lax.rsqrt(variance + EPS)


def rotary_tables(pos_row, head):
    pos = jnp.transpose(jnp.broadcast_to(pos_row.astype(F32), (CHUNK, LANES)))
    dim = iota((CHUNK, LANES), 1) % head
    half = head // 8
    freq = np.float64(10000.0) ** (-2.0 * np.arange(half) / (2 * half))
    which = dim % half
    inv = jnp.full((CHUNK, LANES), np.float32(freq[0]), F32)
    for i in range(1, half):
        inv = jnp.where(which == i, np.float32(freq[i]), inv)
    angle = pos * inv
    cos_a = jnp.cos(angle)
    sin_a = jnp.sin(angle)
    cos_t = jnp.where(dim < 2 * half, cos_a, 1.0)
    sin_lo = jnp.where(dim < half, -sin_a, 0.0)
    sin_hi = jnp.where((dim >= half) & (dim < 2 * half), sin_a, 0.0)
    return pos, cos_t, sin_lo, sin_hi


def rotate(x, tables, half):
    cos_t, sin_lo, sin_hi = tables
    up = pltpu.roll(x, LANES - half, 1)
    down = pltpu.roll(x, half, 1)
    return x * cos_t + up * sin_lo + down * sin_hi


def attend_kernel(layer, num_rows, head, *refs):
    (pos_ref, pos_sm, hid_any, gain_ref, bias_ref, w_any, b_ref, k_in, v_in) = refs[:9]
    refs = refs[9:]
    if layer > 0:
        refs = refs[2:]
    (k_out, v_out, ctx_ref, hid_s, w_s, q_s, pos_s, kn_s, vn_s, k_buf, v_buf, rd_sem, wr_sem, in_sem) = refs
    num_blocks = num_rows // BLOCK
    per_chunk = CHUNK // BLOCK

    def reads(blk, slot):
        rows = pl.ds(blk * BLOCK, BLOCK)
        return (pltpu.make_async_copy(k_in.at[layer, rows], k_buf.at[slot], rd_sem.at[0, slot]),
                pltpu.make_async_copy(v_in.at[layer, rows], v_buf.at[slot], rd_sem.at[1, slot]))

    def writes(blk, slot):
        rows = pl.ds(blk * BLOCK, BLOCK)
        return (pltpu.make_async_copy(k_buf.at[slot], k_out.at[layer, rows], wr_sem.at[0, slot]),
                pltpu.make_async_copy(v_buf.at[slot], v_out.at[layer, rows], wr_sem.at[1, slot]))

    hid_copy = pltpu.make_async_copy(hid_any, hid_s, in_sem.at[0])
    w_copy = pltpu.make_async_copy(w_any.at[layer], w_s, in_sem.at[1])
    hid_copy.start()
    w_copy.start()
    for blk in range(SLOTS):
        for copy in reads(blk, blk):
            copy.start()
    hid_copy.wait()
    w_copy.wait()

    lane = iota((CHUNK, LANES), 1)
    low = lane < head

    @pl.loop(0, num_rows // CHUNK)
    def _(c):
        rows = pl.ds(pl.multiple_of(c * CHUNK, CHUNK), CHUNK)
        pos, *tables = rotary_tables(pos_ref[pl.ds(c, 1), :], head)
        pos_s[rows, :] = pos
        normed = normalize(hid_s[rows, :].astype(F32))
        attn_in = (normed * gain_ref[layer:layer + 1, :] + bias_ref[layer:layer + 1, :]).astype(BF)
        qkv = jnp.dot(attn_in, w_s[...], preferred_element_type=F32) + b_ref[layer:layer + 1, :].astype(F32)
        qkv = qkv.astype(BF).astype(F32)
        one, two, three = qkv[:, :LANES], qkv[:, LANES:2 * LANES], qkv[:, 2 * LANES:]
        query = jnp.where(low, one, two)
        key = pltpu.roll(jnp.where(low, three, one), head, 1)
        value = jnp.where(low, two, three)
        q_s[rows, :] = rotate(query, tables, head // 8).astype(BF).astype(F32)
        key_t = jnp.transpose(rotate(key, tables, head // 8).astype(BF).astype(F32))
        val_t = jnp.transpose(value)
        for i in range(per_chunk):
            kn_s[c * per_chunk + i] = (pltpu.roll(key_t, (LANES - i * BLOCK) % LANES, 1) if i else key_t).astype(kn_s.dtype)
            vn_s[c * per_chunk + i] = (pltpu.roll(val_t, (LANES - i * BLOCK) % LANES, 1) if i else val_t).astype(vn_s.dtype)

    scale = head ** -0.5
    sub16 = iota((16, LANES), 0) % 8
    lane16 = iota((16, LANES), 1)
    lane8 = iota((8, LANES), 1)
    even = (sub16 % 2) == 0
    first = sub16 < 4
    upper = (sub16 % 4) < 2

    def merged(buf, new_s, slot, blk, j, hit):
        shift = lax.rem(pos_sm[blk * BLOCK + j] + (LANES - j), LANES)
        col = pltpu.roll(new_s[blk], shift, 1).astype(BF)
        out = jnp.where(hit, col, buf[slot, j])
        buf[slot, j] = out
        return out

    def square(tiles):
        return jnp.concatenate([jnp.concatenate(tiles[:2], 1), jnp.concatenate(tiles[2:], 1)], 0)

    @pl.loop(0, num_blocks)
    def _(blk):
        slot = lax.rem(blk, SLOTS)

        @pl.when((blk + AHEAD >= SLOTS) & (blk + AHEAD < num_blocks))
        def _():
            ahead = blk + AHEAD
            ahead_slot = lax.rem(ahead, SLOTS)
            for copy in writes(ahead - SLOTS, ahead_slot):
                copy.wait()
            for copy in reads(ahead, ahead_slot):
                copy.start()

        for copy in reads(blk, slot):
            copy.wait()

        base = pl.multiple_of(blk * BLOCK, BLOCK)
        for g in range(BLOCK // 8):
            rows = pl.ds(base + 8 * g, 8)
            q8 = q_s[rows, :]
            p8 = pos_s[rows, :]
            hits = [lane.astype(BF) == jnp.broadcast_to(p8[j:j + 1, :], (LANES, LANES)).astype(BF) for j in range(8)]
            q16 = jnp.concatenate([jnp.where(lane8 < head, q8, 0.0), jnp.where(lane8 < head, 0.0, q8)], 0)
            p16 = jnp.concatenate([p8, p8], 0)
            scores = []
            for t in range(2):
                keys = square([merged(k_buf, kn_s, slot, blk, 8 * g + 4 * t + i, hits[4 * t + i]) for i in range(4)])
                mine = first if t == 0 else ~first
                lhs = jnp.concatenate([jnp.where(mine & upper, q16, 0.0), jnp.where(mine & ~upper, q16, 0.0)], 1).astype(BF)
                out = jnp.dot(lhs, keys, preferred_element_type=F32)
                scores.append(jnp.where(even, out[:, :LANES], out[:, LANES:]))
            s = jnp.where(first, scores[0], scores[1]) * scale
            s = jnp.where(lane16.astype(F32) <= p16, s, -1e30)
            e = jnp.exp(s - jnp.max(s, axis=-1, keepdims=True))
            prob = e / jnp.sum(e, axis=-1, keepdims=True)
            lhs = jnp.concatenate([jnp.where(even, prob, 0.0), jnp.where(even, 0.0, prob)], 1).astype(BF)
            ctx = []
            for t in range(2):
                vals = square([merged(v_buf, vn_s, slot, blk, 8 * g + 4 * t + i, hits[4 * t + i]) for i in range(4)])
                out = lax.dot_general(lhs, vals, (((1,), (1,)), ((), ())), preferred_element_type=F32)
                ctx.append(jnp.where(upper, out[:, :LANES], out[:, LANES:]))
            c16 = jnp.where(first, ctx[0], ctx[1])
            ctx_ref[rows, :] = jnp.where(lane8 < head, c16[:8], c16[8:])

        for copy in writes(blk, slot):
            copy.start()

    for blk in range(num_blocks - SLOTS, num_blocks):
        for copy in writes(blk, blk % SLOTS):
            copy.wait()


def attend(layer, positions, hidden, gain, bias, w_qkv, b_qkv, k_cache, v_cache, prev):
    num_rows, width = hidden.shape
    _, _, inner, slots = k_cache.shape
    head = inner // 2
    num_blocks = num_rows // BLOCK
    vmem = pl.BlockSpec(memory_space=pltpu.VMEM)
    anyspace = pl.BlockSpec(memory_space=pl.ANY)
    operands = [positions, positions.reshape(-1), hidden, gain, bias, w_qkv, b_qkv, k_cache, v_cache]
    specs = [vmem, pl.BlockSpec(memory_space=pltpu.SMEM), anyspace, vmem, vmem, anyspace, vmem, anyspace, anyspace]
    aliases = {}
    if prev is not None:
        operands += list(prev)
        specs += [anyspace, anyspace]
        aliases = {9: 0, 10: 1}
    cache = jax.ShapeDtypeStruct(k_cache.shape, BF)
    return pl.pallas_call(
        functools.partial(attend_kernel, layer, num_rows, head),
        out_shape=(cache, cache, jax.ShapeDtypeStruct((num_rows, inner), F32)),
        in_specs=specs,
        out_specs=(anyspace, anyspace, vmem),
        scratch_shapes=[
            pltpu.VMEM((num_rows, width), BF),
            pltpu.VMEM(w_qkv.shape[1:], BF),
            pltpu.VMEM((num_rows, LANES), F32),
            pltpu.VMEM((num_rows, LANES), F32),
            pltpu.VMEM((num_blocks, LANES, LANES), F32),
            pltpu.VMEM((num_blocks, LANES, LANES), F32),
            pltpu.VMEM((SLOTS, BLOCK, inner, slots), BF),
            pltpu.VMEM((SLOTS, BLOCK, inner, slots), BF),
            pltpu.SemaphoreType.DMA((2, SLOTS)),
            pltpu.SemaphoreType.DMA((2, SLOTS)),
            pltpu.SemaphoreType.DMA((2,)),
        ],
        input_output_aliases=aliases,
        compiler_params=pltpu.CompilerParams(vmem_limit_bytes=56 * 1024 * 1024),
        name=f"attend{layer}",
    )(*operands)


def combine_kernel(layer, num_rows, hid_ref, ctx_ref, gain_ref, bias_ref, w_out_any, w_up_any, b_up_ref, w_down_any, b_out_ref, b_down_ref,
                   out_ref, w_out, w_up, w_down, part, half, pair_in, quad_in, final, in_sem,
                   pair_send, pair_recv, quad_send, quad_recv, gather_send, gather_recv, fwd_send, fwd_recv):
    me = lax.axis_index("tp")
    core = lax.rem(me, 2)
    chip = lax.div(me, 2)
    partner = me + 1 - 2 * core
    others = []
    for k in range(1, 4):
        x = lax.rem(chip, 2)
        y = lax.div(chip, 2)
        ox = 1 - x if k & 1 else x
        oy = 1 - y if k & 2 else y
        others.append(2 * oy + ox)
    num_chunks = num_rows // CHUNK
    half_rows = CHUNK // 2
    piece = CHUNK // 8

    weights = [pltpu.make_async_copy(src.at[layer], dst, in_sem.at[i])
               for i, (src, dst) in enumerate([(w_up_any, w_up), (w_down_any, w_down), (w_out_any, w_out)])]
    for copy in weights:
        copy.start()

    barrier = pltpu.get_barrier_semaphore()
    peers = [partner] + [2 * o + core for o in others]
    for peer in peers:
        pl.semaphore_signal(barrier, inc=1, device_id={"tp": peer}, device_id_type=MESH)

    def remote(src, dst, send, recv, device):
        return pltpu.make_async_remote_copy(src_ref=src, dst_ref=dst, send_sem=send, recv_sem=recv,
                                            device_id={"tp": device}, device_id_type=MESH)

    def pair_copy(c):
        start = pl.multiple_of((1 - core) * half_rows, half_rows)
        return remote(part.at[c, pl.ds(start, half_rows)], pair_in.at[c], pair_send.at[c], pair_recv.at[c], partner)

    def quad_copy(c, k):
        start = pl.multiple_of(others[k] * piece, piece)
        return remote(half.at[c, pl.ds(start, piece)], quad_in.at[c, k], quad_send.at[c, k], quad_recv.at[c, k], 2 * others[k] + core)

    def piece_rows(c, owner_core, owner_chip):
        return pl.ds(pl.multiple_of(c * CHUNK + owner_core * half_rows + owner_chip * piece, piece), piece)

    def gather_copy(c, k):
        rows = piece_rows(c, core, chip)
        return remote(final.at[rows], final.at[rows], gather_send.at[c, k], gather_recv.at[c, k], 2 * others[k] + core)

    def fwd_copy(c):
        rows = pl.ds(pl.multiple_of(c * CHUNK + core * half_rows, half_rows), half_rows)
        return remote(final.at[rows], final.at[rows], fwd_send.at[c], fwd_recv.at[c], partner)

    def compute(c):
        rows = pl.ds(c * CHUNK, CHUNK)
        normed = normalize(hid_ref[rows, :].astype(F32))
        mlp_in = (normed * gain_ref[layer:layer + 1, :] + bias_ref[layer:layer + 1, :]).astype(BF)
        up = jnp.dot(mlp_in, w_up[...], preferred_element_type=F32) + b_up_ref[layer:layer + 1, :].astype(F32)
        act = (0.5 * up * (1.0 + lax.erf(up * np.float32(np.sqrt(0.5))))).astype(BF)
        total = jnp.dot(act, w_down[...], preferred_element_type=F32)
        total = total + jnp.dot(ctx_ref[rows, :].astype(BF), w_out[...], preferred_element_type=F32)
        part[c] = total.astype(BF)

    def pair_done(c):
        pair_copy(c).wait()
        mine = pl.ds(pl.multiple_of(core * half_rows, half_rows), half_rows)
        half[c] = (part[c, mine, :].astype(F32) + pair_in[c].astype(F32)).astype(BF)

    def quad_done(c):
        for k in range(3):
            quad_copy(c, k).wait()
        mine = pl.ds(pl.multiple_of(chip * piece, piece), piece)
        rows = piece_rows(c, core, chip)
        total = hid_ref[rows, :].astype(F32) + half[c, mine, :].astype(F32)
        for k in range(3):
            total = total + quad_in[c, k].astype(F32)
        total = total + b_out_ref[layer:layer + 1, :].astype(F32) + b_down_ref[layer:layer + 1, :].astype(F32)
        final[rows, :] = total.astype(BF)

    for copy in weights:
        copy.wait()
    for step in range(num_chunks + 4):
        if step < num_chunks:
            compute(step)
            if step == 0:
                pl.semaphore_wait(barrier, len(peers))
            pair_copy(step).start()
        if 0 <= step - 1 < num_chunks:
            pair_done(step - 1)
            for k in range(3):
                quad_copy(step - 1, k).start()
        if 0 <= step - 2 < num_chunks:
            quad_done(step - 2)
            for k in range(3):
                gather_copy(step - 2, k).start()
        if 0 <= step - 3 < num_chunks:
            for k in range(3):
                gather_copy(step - 3, k).wait()
            fwd_copy(step - 3).start()
        if 0 <= step - 4 < num_chunks:
            fwd_copy(step - 4).wait()
            rows = pl.ds((step - 4) * CHUNK, CHUNK)
            out_ref[rows, :] = final[rows, :]


def combine(layer, hidden, ctx, gain, bias, w_out, w_up, b_up, w_down, b_out, b_down):
    num_rows, width = hidden.shape
    num_chunks = num_rows // CHUNK
    vmem = pl.BlockSpec(memory_space=pltpu.VMEM)
    anyspace = pl.BlockSpec(memory_space=pl.ANY)
    dma = pltpu.SemaphoreType.DMA
    return pl.pallas_call(
        functools.partial(combine_kernel, layer, num_rows),
        out_shape=jax.ShapeDtypeStruct((num_rows, width), BF),
        in_specs=[vmem, vmem, vmem, vmem, anyspace, anyspace, vmem, anyspace, vmem, vmem],
        out_specs=vmem,
        scratch_shapes=[
            pltpu.VMEM(w_out.shape[1:], BF),
            pltpu.VMEM(w_up.shape[1:], BF),
            pltpu.VMEM(w_down.shape[1:], BF),
            pltpu.VMEM((num_chunks, CHUNK, width), BF),
            pltpu.VMEM((num_chunks, CHUNK // 2, width), BF),
            pltpu.VMEM((num_chunks, CHUNK // 2, width), BF),
            pltpu.VMEM((num_chunks, 3, CHUNK // 8, width), BF),
            pltpu.VMEM((num_rows, width), BF),
            dma((3,)),
            dma((num_chunks,)), dma((num_chunks,)),
            dma((num_chunks, 3)), dma((num_chunks, 3)),
            dma((num_chunks, 3)), dma((num_chunks, 3)),
            dma((num_chunks,)), dma((num_chunks,)),
        ],
        compiler_params=pltpu.CompilerParams(collective_id=layer, has_side_effects=True, vmem_limit_bytes=48 * 1024 * 1024),
        name=f"combine{layer}",
    )(hidden, ctx, gain, bias, w_out, w_up, b_up, w_down, b_out, b_down)


def solution(mesh):
    cache_spec = P(None, 'dp', 'tp', None, None)
    rep_spec = P(None, None)
    in_specs = (P('dp', None), P('dp'), rep_spec, rep_spec, rep_spec, rep_spec,
                P(None, None, 'tp'), P(None, 'tp'), P(None, 'tp', None), rep_spec,
                P(None, None, 'tp'), P(None, 'tp'), P(None, 'tp', None), rep_spec,
                cache_spec, cache_spec)
    out_specs = (P('dp', None), cache_spec, cache_spec)

    def local(hidden, positions, ln1_gain, ln1_bias, ln2_gain, ln2_bias, w_qkv, b_qkv, w_out, b_out, w_up, b_up, w_down, b_down, k_cache, v_cache):
        num_layers, num_rows, heads_local, slots, head_dim = k_cache.shape
        flat = (num_layers, num_rows, heads_local * head_dim, slots)
        k_flat = jnp.swapaxes(k_cache, 3, 4).reshape(flat)
        v_flat = jnp.swapaxes(v_cache, 3, 4).reshape(flat)
        pos = positions.reshape(num_rows // CHUNK, CHUNK)
        prev = None
        for layer in range(num_layers):
            k_out, v_out, ctx = attend(layer, pos, hidden, ln1_gain, ln1_bias, w_qkv, b_qkv, k_flat, v_flat, prev)
            prev = (k_out, v_out)
            hidden = combine(layer, hidden, ctx, ln2_gain, ln2_bias, w_out, w_up, b_up, w_down, b_out, b_down)
        shape = (num_layers, num_rows, heads_local, head_dim, slots)
        return hidden, jnp.swapaxes(prev[0].reshape(shape), 3, 4), jnp.swapaxes(prev[1].reshape(shape), 3, 4)

    return jax.shard_map(local, mesh=mesh, in_specs=in_specs, out_specs=out_specs, check_vma=False)
```

```python
import functools

import jax
import jax.numpy as jnp
import numpy as np
from jax import lax
from jax.experimental import pallas as pl
from jax.experimental.pallas import tpu as pltpu
from jax.sharding import PartitionSpec as P

EPS = 1e-5
BF = jnp.bfloat16
F32 = jnp.float32
MESH = pl.DeviceIdType.MESH
LANES = 128
BLOCK = 32
SLOTS = 12
AHEAD = 8
GROUP = 16
CHUNK = 128


def iota(shape, dim):
    return lax.broadcasted_iota(jnp.int32, shape, dim)


def normalize(hid):
    mean_val = jnp.mean(hid, axis=-1, keepdims=True)
    centered = hid - mean_val
    variance = jnp.mean(centered * centered, axis=-1, keepdims=True)
    return centered * lax.rsqrt(variance + EPS)


def rotary_tables(pos_row, head):
    pos = jnp.transpose(jnp.broadcast_to(pos_row.astype(F32), (CHUNK, LANES)))
    dim = iota((CHUNK, LANES), 1) % head
    half = head // 8
    freq = np.float64(10000.0) ** (-2.0 * np.arange(half) / (2 * half))
    which = dim % half
    inv = jnp.full((CHUNK, LANES), np.float32(freq[0]), F32)
    for i in range(1, half):
        inv = jnp.where(which == i, np.float32(freq[i]), inv)
    angle = pos * inv
    cos_a = jnp.cos(angle)
    sin_a = jnp.sin(angle)
    cos_t = jnp.where(dim < 2 * half, cos_a, 1.0)
    sin_lo = jnp.where(dim < half, -sin_a, 0.0)
    sin_hi = jnp.where((dim >= half) & (dim < 2 * half), sin_a, 0.0)
    return pos, cos_t, sin_lo, sin_hi


def rotate(x, tables, half):
    cos_t, sin_lo, sin_hi = tables
    up = pltpu.roll(x, LANES - half, 1)
    down = pltpu.roll(x, half, 1)
    return x * cos_t + up * sin_lo + down * sin_hi


def attend_kernel(layer, num_rows, head, *refs):
    (pos_ref, pos_sm, hid_s, gain_ref, bias_ref, w_ref, b_ref, k_in, v_in) = refs[:9]
    refs = refs[9:]
    if layer > 0:
        refs = refs[2:]
    (k_out, v_out, ctx_ref, q_s, pos_s, kn_s, vn_s, k_buf, v_buf, rd_sem, wr_sem) = refs
    num_blocks = num_rows // BLOCK
    per_chunk = CHUNK // BLOCK

    def reads(blk, slot):
        rows = pl.ds(blk * BLOCK, BLOCK)
        return (pltpu.make_async_copy(k_in.at[layer, rows], k_buf.at[slot], rd_sem.at[0, slot]),
                pltpu.make_async_copy(v_in.at[layer, rows], v_buf.at[slot], rd_sem.at[1, slot]))

    def writes(blk, slot):
        rows = pl.ds(blk * BLOCK, BLOCK)
        return (pltpu.make_async_copy(k_buf.at[slot], k_out.at[layer, rows], wr_sem.at[0, slot]),
                pltpu.make_async_copy(v_buf.at[slot], v_out.at[layer, rows], wr_sem.at[1, slot]))

    for blk in range(SLOTS):
        for copy in reads(blk, blk):
            copy.start(priority=1)

    lane = iota((CHUNK, LANES), 1)
    low = lane < head

    @pl.loop(0, num_rows // CHUNK)
    def _(c):
        rows = pl.ds(pl.multiple_of(c * CHUNK, CHUNK), CHUNK)
        pos, *tables = rotary_tables(pos_ref[pl.ds(c, 1), :], head)
        pos_s[rows, :] = pos
        normed = normalize(hid_s[rows, :].astype(F32))
        attn_in = (normed * gain_ref[layer:layer + 1, :] + bias_ref[layer:layer + 1, :]).astype(BF)
        qkv = jnp.dot(attn_in, w_ref[layer], preferred_element_type=F32) + b_ref[layer:layer + 1, :].astype(F32)
        qkv = qkv.astype(BF).astype(F32)
        one, two, three = qkv[:, :LANES], qkv[:, LANES:2 * LANES], qkv[:, 2 * LANES:]
        query = jnp.where(low, one, two)
        key = pltpu.roll(jnp.where(low, three, one), head, 1)
        value = jnp.where(low, two, three)
        q_s[rows, :] = rotate(query, tables, head // 8).astype(BF).astype(F32)
        key_t = jnp.transpose(rotate(key, tables, head // 8).astype(BF).astype(F32))
        val_t = jnp.transpose(value)
        for i in range(CHUNK // GROUP):
            kn_s[c * (CHUNK // GROUP) + i] = (pltpu.roll(key_t, LANES - i * GROUP, 1) if i else key_t).astype(kn_s.dtype)
            vn_s[c * (CHUNK // GROUP) + i] = (pltpu.roll(val_t, LANES - i * GROUP, 1) if i else val_t).astype(vn_s.dtype)

    scale = head ** -0.5
    sub16 = iota((16, LANES), 0) % 8
    lane16 = iota((16, LANES), 1)
    row16 = iota((16, LANES), 0)
    lane8 = iota((8, LANES), 1)
    even = (sub16 % 2) == 0
    first = sub16 < 4
    upper = (sub16 % 4) < 2

    def merged(buf, cols, slot, j, hit):
        out = jnp.where(hit, cols[:, j % 2 * LANES:(j % 2 + 1) * LANES], buf[slot, j])
        buf[slot, j] = out
        return out

    def pair_cols(new_s, blk, j, p8):
        tile = new_s[blk * (BLOCK // GROUP) + j // GROUP]
        if layer == 0:
            hot = [jnp.where((row16 == (j + i) % GROUP) & (lane16 == p8[(j + i) % 8:(j + i) % 8 + 1, :].astype(jnp.int32)), 1.0, 0.0) for i in range(2)]
            hot = jnp.concatenate(hot, 1).astype(BF)
            return jnp.dot(tile[:, :GROUP].astype(BF), hot, preferred_element_type=F32).astype(BF)
        cols = []
        for i in range(2):
            shift = lax.rem(pos_sm[blk * BLOCK + j + i] + (LANES - (j + i) % GROUP), LANES)
            cols.append(pltpu.roll(tile, shift, 1).astype(BF))
        return jnp.concatenate(cols, 1)

    def quad(buf, new_s, slot, blk, j, hits, p8):
        tiles = []
        for i in (0, 2):
            cols = pair_cols(new_s, blk, j + i, p8)
            tiles += [merged(buf, cols, slot, j + i, hits[i]), merged(buf, cols, slot, j + i + 1, hits[i + 1])]
        return jnp.concatenate([jnp.concatenate(tiles[:2], 1), jnp.concatenate(tiles[2:], 1)], 0)

    @pl.loop(0, num_blocks)
    def _(blk):
        slot = lax.rem(blk, SLOTS)

        @pl.when((blk + AHEAD >= SLOTS) & (blk + AHEAD < num_blocks))
        def _():
            ahead = blk + AHEAD
            ahead_slot = lax.rem(ahead, SLOTS)
            for copy in writes(ahead - SLOTS, ahead_slot):
                copy.wait()
            for copy in reads(ahead, ahead_slot):
                copy.start(priority=1)

        for copy in reads(blk, slot):
            copy.wait()

        base = pl.multiple_of(blk * BLOCK, BLOCK)
        for g in range(BLOCK // 8):
            rows = pl.ds(base + 8 * g, 8)
            q8 = q_s[rows, :]
            p8 = pos_s[rows, :]
            hits = [lane.astype(BF) == jnp.broadcast_to(p8[j:j + 1, :], (LANES, LANES)).astype(BF) for j in range(8)]
            q16 = jnp.concatenate([jnp.where(lane8 < head, q8, 0.0), jnp.where(lane8 < head, 0.0, q8)], 0)
            p16 = jnp.concatenate([p8, p8], 0)
            scores = []
            for t in range(2):
                keys = quad(k_buf, kn_s, slot, blk, 8 * g + 4 * t, hits[4 * t:4 * t + 4], p8)
                mine = first if t == 0 else ~first
                lhs = jnp.concatenate([jnp.where(mine & upper, q16, 0.0), jnp.where(mine & ~upper, q16, 0.0)], 1).astype(BF)
                out = jnp.dot(lhs, keys, preferred_element_type=F32)
                scores.append(jnp.where(even, out[:, :LANES], out[:, LANES:]))
            s = jnp.where(first, scores[0], scores[1]) * scale
            s = jnp.where(lane16.astype(F32) <= p16, s, -1e30)
            e = jnp.exp(s - jnp.max(s, axis=-1, keepdims=True))
            prob = e / jnp.sum(e, axis=-1, keepdims=True)
            lhs = jnp.concatenate([jnp.where(even, prob, 0.0), jnp.where(even, 0.0, prob)], 1).astype(BF)
            ctx = []
            for t in range(2):
                vals = quad(v_buf, vn_s, slot, blk, 8 * g + 4 * t, hits[4 * t:4 * t + 4], p8)
                out = lax.dot_general(lhs, vals, (((1,), (1,)), ((), ())), preferred_element_type=F32)
                ctx.append(jnp.where(upper, out[:, :LANES], out[:, LANES:]))
            c16 = jnp.where(first, ctx[0], ctx[1])
            ctx_ref[rows, :] = jnp.where(lane8 < head, c16[:8], c16[8:])

        for copy in writes(blk, slot):
            copy.start()

    for blk in range(num_blocks - SLOTS, num_blocks):
        for copy in writes(blk, blk % SLOTS):
            copy.wait()


def attend(layer, positions, hidden, gain, bias, w_qkv, b_qkv, k_cache, v_cache, prev):
    num_rows, width = hidden.shape
    _, _, inner, slots = k_cache.shape
    head = inner // 2
    num_blocks = num_rows // BLOCK
    vmem = pl.BlockSpec(memory_space=pltpu.VMEM)
    anyspace = pl.BlockSpec(memory_space=pl.ANY)
    operands = [positions, positions.reshape(-1), hidden, gain, bias, w_qkv, b_qkv, k_cache, v_cache]
    specs = [vmem, pl.BlockSpec(memory_space=pltpu.SMEM), vmem, vmem, vmem, vmem, vmem, anyspace, anyspace]
    aliases = {}
    if prev is not None:
        operands += list(prev)
        specs += [anyspace, anyspace]
        aliases = {9: 0, 10: 1}
    cache = jax.ShapeDtypeStruct(k_cache.shape, BF)
    return pl.pallas_call(
        functools.partial(attend_kernel, layer, num_rows, head),
        out_shape=(cache, cache, jax.ShapeDtypeStruct((num_rows, inner), F32)),
        in_specs=specs,
        out_specs=(anyspace, anyspace, vmem),
        scratch_shapes=[
            pltpu.VMEM((num_rows, LANES), F32),
            pltpu.VMEM((num_rows, LANES), F32),
            pltpu.VMEM((num_rows // GROUP, LANES, LANES), F32 if layer else BF),
            pltpu.VMEM((num_rows // GROUP, LANES, LANES), F32 if layer else BF),
            pltpu.VMEM((SLOTS, BLOCK, inner, slots), BF),
            pltpu.VMEM((SLOTS, BLOCK, inner, slots), BF),
            pltpu.SemaphoreType.DMA((2, SLOTS)),
            pltpu.SemaphoreType.DMA((2, SLOTS)),
        ],
        input_output_aliases=aliases,
        compiler_params=pltpu.CompilerParams(vmem_limit_bytes=44 * 1024 * 1024),
        name=f"attend{layer}",
    )(*operands)


def combine_kernel(layer, num_rows, hid_ref, ctx_ref, gain_ref, bias_ref, w_out, w_up, b_up_ref, w_down, b_out_ref, b_down_ref,
                   out_ref, part, half, pair_in, quad_in, final,
                   pair_send, pair_recv, quad_send, quad_recv, gather_send, gather_recv, fwd_send, fwd_recv):
    me = lax.axis_index("tp")
    core = lax.rem(me, 2)
    chip = lax.div(me, 2)
    partner = me + 1 - 2 * core
    others = []
    for k in range(1, 4):
        x = lax.rem(chip, 2)
        y = lax.div(chip, 2)
        ox = 1 - x if k & 1 else x
        oy = 1 - y if k & 2 else y
        others.append(2 * oy + ox)
    num_chunks = num_rows // CHUNK
    half_rows = CHUNK // 2
    piece = CHUNK // 8

    barrier = pltpu.get_barrier_semaphore()
    peers = [partner] + [2 * o + core for o in others]
    for peer in peers:
        pl.semaphore_signal(barrier, inc=1, device_id={"tp": peer}, device_id_type=MESH)

    def remote(src, dst, send, recv, device):
        return pltpu.make_async_remote_copy(src_ref=src, dst_ref=dst, send_sem=send, recv_sem=recv,
                                            device_id={"tp": device}, device_id_type=MESH)

    def pair_copy(c):
        start = pl.multiple_of((1 - core) * half_rows, half_rows)
        return remote(part.at[c, pl.ds(start, half_rows)], pair_in.at[c], pair_send.at[c], pair_recv.at[c], partner)

    def quad_copy(c, k):
        start = pl.multiple_of(others[k] * piece, piece)
        return remote(half.at[c, pl.ds(start, piece)], quad_in.at[c, k], quad_send.at[c, k], quad_recv.at[c, k], 2 * others[k] + core)

    def piece_rows(c, owner_core, owner_chip):
        return pl.ds(pl.multiple_of(c * CHUNK + owner_core * half_rows + owner_chip * piece, piece), piece)

    def gather_copy(c, k):
        rows = piece_rows(c, core, chip)
        return remote(final.at[rows], final.at[rows], gather_send.at[c, k], gather_recv.at[c, k], 2 * others[k] + core)

    def fwd_copy(c):
        rows = pl.ds(pl.multiple_of(c * CHUNK + core * half_rows, half_rows), half_rows)
        return remote(final.at[rows], final.at[rows], fwd_send.at[c], fwd_recv.at[c], partner)

    def compute(c):
        rows = pl.ds(c * CHUNK, CHUNK)
        normed = normalize(hid_ref[rows, :].astype(F32))
        mlp_in = (normed * gain_ref[layer:layer + 1, :] + bias_ref[layer:layer + 1, :]).astype(BF)
        up = jnp.dot(mlp_in, w_up[layer], preferred_element_type=F32) + b_up_ref[layer:layer + 1, :].astype(F32)
        act = (0.5 * up * (1.0 + lax.erf(up * np.float32(np.sqrt(0.5))))).astype(BF)
        total = jnp.dot(act, w_down[layer], preferred_element_type=F32)
        total = total + jnp.dot(ctx_ref[rows, :].astype(BF), w_out[layer], preferred_element_type=F32)
        part[c] = total.astype(BF)

    def pair_done(c):
        pair_copy(c).wait()
        mine = pl.ds(pl.multiple_of(core * half_rows, half_rows), half_rows)
        half[c] = (part[c, mine, :].astype(F32) + pair_in[c].astype(F32)).astype(BF)

    def quad_done(c):
        for k in range(3):
            quad_copy(c, k).wait()
        mine = pl.ds(pl.multiple_of(chip * piece, piece), piece)
        rows = piece_rows(c, core, chip)
        total = hid_ref[rows, :].astype(F32) + half[c, mine, :].astype(F32)
        for k in range(3):
            total = total + quad_in[c, k].astype(F32)
        total = total + b_out_ref[layer:layer + 1, :].astype(F32) + b_down_ref[layer:layer + 1, :].astype(F32)
        final[rows, :] = total.astype(BF)

    for step in range(num_chunks + 4):
        if step < num_chunks:
            compute(step)
            if step == 0:
                pl.semaphore_wait(barrier, len(peers))
            pair_copy(step).start()
        if 0 <= step - 1 < num_chunks:
            pair_done(step - 1)
            for k in range(3):
                quad_copy(step - 1, k).start()
        if 0 <= step - 2 < num_chunks:
            quad_done(step - 2)
            for k in range(3):
                gather_copy(step - 2, k).start()
        if 0 <= step - 3 < num_chunks:
            for k in range(3):
                gather_copy(step - 3, k).wait()
            fwd_copy(step - 3).start()
        if 0 <= step - 4 < num_chunks:
            fwd_copy(step - 4).wait()
            rows = pl.ds((step - 4) * CHUNK, CHUNK)
            out_ref[rows, :] = final[rows, :]


def combine(layer, hidden, ctx, gain, bias, w_out, w_up, b_up, w_down, b_out, b_down):
    num_rows, width = hidden.shape
    num_chunks = num_rows // CHUNK
    vmem = pl.BlockSpec(memory_space=pltpu.VMEM)
    dma = pltpu.SemaphoreType.DMA
    return pl.pallas_call(
        functools.partial(combine_kernel, layer, num_rows),
        out_shape=jax.ShapeDtypeStruct((num_rows, width), BF),
        in_specs=[vmem] * 10,
        out_specs=vmem,
        scratch_shapes=[
            pltpu.VMEM((num_chunks, CHUNK, width), BF),
            pltpu.VMEM((num_chunks, CHUNK // 2, width), BF),
            pltpu.VMEM((num_chunks, CHUNK // 2, width), BF),
            pltpu.VMEM((num_chunks, 3, CHUNK // 8, width), BF),
            pltpu.VMEM((num_rows, width), BF),
            dma((num_chunks,)), dma((num_chunks,)),
            dma((num_chunks, 3)), dma((num_chunks, 3)),
            dma((num_chunks, 3)), dma((num_chunks, 3)),
            dma((num_chunks,)), dma((num_chunks,)),
        ],
        compiler_params=pltpu.CompilerParams(collective_id=layer, has_side_effects=True, vmem_limit_bytes=20 * 1024 * 1024),
        name=f"combine{layer}",
    )(hidden, ctx, gain, bias, w_out, w_up, b_up, w_down, b_out, b_down)


def solution(mesh):
    cache_spec = P(None, 'dp', 'tp', None, None)
    rep_spec = P(None, None)
    in_specs = (P('dp', None), P('dp'), rep_spec, rep_spec, rep_spec, rep_spec,
                P(None, None, 'tp'), P(None, 'tp'), P(None, 'tp', None), rep_spec,
                P(None, None, 'tp'), P(None, 'tp'), P(None, 'tp', None), rep_spec,
                cache_spec, cache_spec)
    out_specs = (P('dp', None), cache_spec, cache_spec)

    def local(hidden, positions, ln1_gain, ln1_bias, ln2_gain, ln2_bias, w_qkv, b_qkv, w_out, b_out, w_up, b_up, w_down, b_down, k_cache, v_cache):
        num_layers, num_rows, heads_local, slots, head_dim = k_cache.shape
        flat = (num_layers, num_rows, heads_local * head_dim, slots)
        k_flat = jnp.swapaxes(k_cache, 3, 4).reshape(flat)
        v_flat = jnp.swapaxes(v_cache, 3, 4).reshape(flat)
        pos = positions.reshape(num_rows // CHUNK, CHUNK)
        prev = None
        for layer in range(num_layers):
            k_out, v_out, ctx = attend(layer, pos, hidden, ln1_gain, ln1_bias, w_qkv, b_qkv, k_flat, v_flat, prev)
            prev = (k_out, v_out)
            hidden = combine(layer, hidden, ctx, ln2_gain, ln2_bias, w_out, w_up, b_up, w_down, b_out, b_down)
        shape = (num_layers, num_rows, heads_local, head_dim, slots)
        return hidden, jnp.swapaxes(prev[0].reshape(shape), 3, 4), jnp.swapaxes(prev[1].reshape(shape), 3, 4)

    return jax.shard_map(local, mesh=mesh, in_specs=in_specs, out_specs=out_specs, check_vma=False)
```
